128 devices in a mesh: rep: 16 (over x_hi, z, core), tp: 8 (over x_lo, y).
Axes of the slice: x: 4 (x_hi: 2, x_lo: 2; x = x_hi * 2 + x_lo), y: 4, z: 4, core: 2. Of those that a mesh axis runs over, the one named last changes fastest.
Arguments:
- hidden: bfloat16 [64, 4608], P('rep'), may hold values from -6 to 6
- positions: int32 [64], P('rep'), may hold values from 1 to 1023
- key_cache: bfloat16 [64, 16, 1024, 128], P('rep', 'tp'), may hold values from -6 to 6
- value_cache: bfloat16 [64, 16, 1024, 128], P('rep', 'tp'), may hold values from -6 to 6
- norm_gain: float32 [4608], replicated, may hold values from 0.1 to 1.9
- q_proj: bfloat16 [4096, 4608], P(('rep', 'tp')), may hold values from -0.09375 to 0.09375
- k_proj: bfloat16 [2048, 4608], P(('rep', 'tp')), may hold values from -0.09375 to 0.09375
- v_proj: bfloat16 [2048, 4608], P(('rep', 'tp')), may hold values from -0.09375 to 0.09375
- o_proj: bfloat16 [4608, 4096], P(('rep', 'tp')), may hold values from -0.09375 to 0.09375
- post_gain: float32 [4608], P('tp'), may hold values from 0.1 to 1.9
Outputs:
- joined_qkv: bfloat16 [4608, 8192], P(None, 'tp')
- wo_heads: bfloat16 [4096, 4608], P('tp')
- attn_out: bfloat16 [64, 4608], P('rep', 'tp')
The draws below stay inside these ranges and needn't reach their ends.
All inputs are finite; a program needn't handle non-finite values.
Results may differ from the reference program's by a relative error of at most 0.008.
Values may be sent and summed in bfloat16 or wider, within the bound.
No kernel may reach another device: no remote copies, remote signals or barrier semaphores. Data moves between devices by JAX's collectives and lax.ppermute only.
A program may use at most 128 MiB of HBM per device.

```python
import jax
import jax.numpy as jnp
from jax import lax

D = 4608
HEADS = 32
KV_HEADS = 16
HEAD_DIM = 128
CTX = 1024
BATCH = 64
QKV_COLS = 8192
N_TP = 8


def touch_ends(entries, own_key, smallest, high):
    index_at = [jax.random.randint(jax.random.fold_in(own_key, axis), (), 0, length) for axis, length in enumerate(entries.shape)]
    main_axis = entries.shape.index(max(entries.shape))
    next_to = index_at[:main_axis] + [(index_at[main_axis] + 1) % entries.shape[main_axis]] + index_at[main_axis + 1:]
    return entries.at[tuple(index_at)].set(smallest).at[tuple(next_to)].set(high)


def block_scale(key, dims, pieces, low, high):
    def one(position, parts):
        draws = jax.random.uniform(jax.random.fold_in(jax.random.fold_in(key, 6), position), (parts,), jnp.float32, low / len(pieces), high / len(pieces))
        return jnp.repeat(jnp.exp(draws), dims[position] // parts).reshape((-1,) + (1,) * (len(dims) - position - 1))

    loudness = one(*pieces[0])
    for cut in pieces[1:]:
        loudness = loudness * one(*cut)
    return loudness


def normal_values(key, shape, deviation, limit, cuts=(), kind=jnp.bfloat16):
    entries = deviation * jax.random.normal(key, shape, jnp.float32)
    if cuts:
        entries = entries * block_scale(key, shape, cuts, -0.22, 0.18)
    return jnp.clip(entries, -limit, limit).astype(kind)


def setup_inputs(seed: int = 0) -> dict:
    arg_keys = jax.random.split(jax.random.key(seed), 11)
    return {
        "hidden": normal_values(arg_keys[0], (BATCH, D), 1.0, 6.0, ((0, 16),)),
        "positions": touch_ends(jax.random.randint(arg_keys[1], (BATCH,), 1, CTX), jax.random.fold_in(arg_keys[1], 1), 1, CTX - 1).astype(jnp.int32),
        "key_cache": normal_values(arg_keys[2], (BATCH, KV_HEADS, CTX, HEAD_DIM), 1.0, 6.0, ((0, 16), (1, 8))),
        "value_cache": normal_values(arg_keys[3], (BATCH, KV_HEADS, CTX, HEAD_DIM), 1.0, 6.0, ((0, 16), (1, 8))),
        "norm_gain": jnp.clip(1.0 + 0.18 * jax.random.normal(arg_keys[4], (D,), jnp.float32), 0.1, 1.9),
        "q_proj": normal_values(arg_keys[5], (HEADS * HEAD_DIM, D), D ** -0.5, 0.09375, ((0, 128),)),
        "k_proj": normal_values(arg_keys[6], (KV_HEADS * HEAD_DIM, D), D ** -0.5, 0.09375, ((0, 128),)),
        "v_proj": normal_values(arg_keys[7], (KV_HEADS * HEAD_DIM, D), D ** -0.5, 0.09375, ((0, 128),)),
        "o_proj": normal_values(arg_keys[8], (D, HEADS * HEAD_DIM), (HEADS * HEAD_DIM) ** -0.5, 0.09375, ((0, 128),)),
        "post_gain": jnp.clip(1.0 + 0.18 * jax.random.normal(arg_keys[9], (D,), jnp.float32), 0.1, 1.9),
    }


score_scale = 144.0 ** (-0.5)
soft_cap = 50.0

def rms_scale(values, gain):
    mean_square = lax.optimization_barrier(jnp.mean(values * values, axis=-1, keepdims=True))
    return values * lax.rsqrt(mean_square + 1e-06) * gain

def rotate(values, positions):
    half = values.shape[-1] // 2
    freq = 10000.0 ** (-2.0 * jnp.arange(half, dtype=jnp.float32) / values.shape[-1])
    angle = positions.astype(jnp.float32)[:, None] * freq[None, :]
    cosine = jnp.cos(angle)[:, None, :]
    sine = jnp.sin(angle)[:, None, :]
    first = values[..., :half]
    second = values[..., half:]
    return jnp.concatenate([first * cosine - second * sine, second * cosine + first * sine], axis=-1)

def reference(hidden, positions, key_cache, value_cache, norm_gain, q_proj, k_proj, v_proj, o_proj, post_gain):
    q_cols = jnp.transpose(q_proj).reshape(D, N_TP, -1)
    k_cols = jnp.transpose(k_proj).reshape(D, N_TP, -1)
    v_cols = jnp.transpose(v_proj).reshape(D, N_TP, -1)
    joined_qkv = jnp.concatenate([q_cols, k_cols, v_cols], axis=2).reshape(D, QKV_COLS)
    wo_heads = jnp.transpose(o_proj)
    normed = rms_scale(hidden.astype(jnp.float32), norm_gain).astype(jnp.bfloat16)
    query = jnp.dot(normed, jnp.transpose(q_proj), preferred_element_type=jnp.float32).reshape(BATCH, HEADS, HEAD_DIM)
    keys_new = jnp.dot(normed, jnp.transpose(k_proj), preferred_element_type=jnp.float32).reshape(BATCH, KV_HEADS, HEAD_DIM)
    values_new = jnp.dot(normed, jnp.transpose(v_proj), preferred_element_type=jnp.float32).reshape(BATCH, KV_HEADS, HEAD_DIM)
    query_rot = rotate(query, positions).astype(jnp.bfloat16)
    rotated_keys = rotate(keys_new, positions).astype(jnp.bfloat16)
    values_rot = values_new.astype(jnp.bfloat16)
    group = HEADS // KV_HEADS
    grouped_heads = query_rot.astype(jnp.float32).reshape(BATCH, KV_HEADS, group, HEAD_DIM)
    scores = jnp.einsum('bkgd,bkld->bkgl', grouped_heads, key_cache.astype(jnp.float32)) * score_scale
    capped = soft_cap * jnp.tanh(scores / soft_cap)
    valid = jnp.arange(CTX, dtype=jnp.int32)[None, :] < positions[:, None]
    weight_raw = jnp.where(valid[:, None, None, :], jnp.exp(capped), 0.0)
    self_score = lax.optimization_barrier(jnp.sum(grouped_heads * rotated_keys.astype(jnp.float32)[:, :, None, :], axis=-1)) * score_scale
    self_raw = jnp.exp(soft_cap * jnp.tanh(self_score / soft_cap))
    denom = lax.optimization_barrier(jnp.sum(weight_raw, axis=-1)) + self_raw
    weights = (weight_raw / denom[..., None]).astype(jnp.bfloat16)
    self_weight = (self_raw / denom).astype(jnp.bfloat16)
    attention = jnp.einsum('bkgl,bkld->bkgd', weights.astype(jnp.float32), value_cache.astype(jnp.float32))
    attention = attention + self_weight.astype(jnp.float32)[..., None] * values_rot.astype(jnp.float32)[:, :, None, :]
    attention = attention.reshape(BATCH, HEADS * HEAD_DIM).astype(jnp.bfloat16)
    projected = jnp.dot(attention, wo_heads, preferred_element_type=jnp.float32)
    attn_out = rms_scale(projected, post_gain).astype(jnp.bfloat16)
    return (joined_qkv, wo_heads, attn_out)
```

```python
import functools

import jax
import jax.numpy as jnp
from jax import lax
from jax.experimental import pallas as pl
from jax.experimental.pallas import tpu as pltpu
from jax.sharding import PartitionSpec as P

score_scale = 144.0 ** (-0.5)
soft_cap = 50.0
AXES = ("rep", "tp")


def flat_index(x, y, z, c):
    x, y, z, c = x % 4, y % 4, z % 4, c % 2
    return ((x // 2) * 8 + z * 2 + c) * 8 + (x % 2) * 4 + y


def moved(value, to):
    pairs = []
    for x in range(4):
        for y in range(4):
            for z in range(4):
                for c in range(2):
                    pairs.append((flat_index(x, y, z, c), flat_index(*to(x, y, z, c))))
    return lax.ppermute(value, AXES, pairs)


SWAPPED = (0, 2, 1, 3)


def chosen(index, options):
    result = options[0]
    for k in range(1, len(options)):
        result = jnp.where(index == k, options[k], result)
    return result


def joined_kernel(table, *refs):
    pieces, out, rows = refs[:8], refs[8], refs[9]
    for i in range(8):
        for t in range(2):
            place = table[2 * i + t]
            q_at = pl.multiple_of(place * 32, 32)
            kv_at = pl.multiple_of(place * 16, 16)
            rows[pl.ds(q_at, 32), :] = pieces[i][t, 0:32, :]
            rows[pl.ds(512 + kv_at, 16), :] = pieces[i][t, 32:48, :]
            rows[pl.ds(768 + kv_at, 16), :] = pieces[i][t, 48:64, :]
    out[...] = jnp.transpose(rows[...])


def joined_columns(table, pieces, chunk):
    _, height, width = pieces[0].shape
    block = pl.BlockSpec((2, height, chunk), lambda d, *_: (0, 0, d))
    total = height * 16
    return pl.pallas_call(
        joined_kernel,
        out_shape=jax.ShapeDtypeStruct((width, total), jnp.bfloat16),
        grid_spec=pltpu.PrefetchScalarGridSpec(
            num_scalar_prefetch=1,
            grid=(width // chunk,),
            in_specs=[block] * 8,
            out_specs=pl.BlockSpec((chunk, total), lambda d, *_: (d, 0)),
            scratch_shapes=[pltpu.VMEM((total, chunk), jnp.bfloat16)],
        ),
        cost_estimate=pl.CostEstimate(
            flops=width * total, bytes_accessed=4 * width * total, transcendentals=0
        ),
        name="joined",
    )(table, *pieces)


def wo_kernel(table, *refs):
    pieces, out, rows = refs[:8], refs[8], refs[9]
    height = pieces[0].shape[1]
    for i in range(8):
        for t in range(2):
            at = pl.multiple_of(table[2 * i + t] * height, 16)
            rows[pl.ds(at, height), :] = pieces[i][t]
    out[...] = jnp.transpose(rows[...])


def wo_rows(table, pieces, chunk):
    _, height, width = pieces[0].shape
    block = pl.BlockSpec((2, height, chunk), lambda d, *_: (0, 0, d))
    total = height * 16
    return pl.pallas_call(
        wo_kernel,
        out_shape=jax.ShapeDtypeStruct((width, total), jnp.bfloat16),
        grid_spec=pltpu.PrefetchScalarGridSpec(
            num_scalar_prefetch=1,
            grid=(width // chunk,),
            in_specs=[block] * 8,
            out_specs=pl.BlockSpec((chunk, total), lambda d, *_: (d, 0)),
            scratch_shapes=[pltpu.VMEM((total, chunk), jnp.bfloat16)],
        ),
        cost_estimate=pl.CostEstimate(
            flops=width * total, bytes_accessed=4 * width * total, transcendentals=0
        ),
        name="wo",
    )(table, *pieces)


def rms_scale(values, gain):
    mean_square = jnp.mean(values * values, axis=-1, keepdims=True)
    return values * lax.rsqrt(mean_square + 1e-06) * gain


def rotate(values, positions):
    half = values.shape[-1] // 2
    freq = 10000.0 ** (-2.0 * jnp.arange(half, dtype=jnp.float32) / values.shape[-1])
    angle = positions.astype(jnp.float32)[:, None] * freq[None, :]
    cosine = jnp.cos(angle)[:, None, :]
    sine = jnp.sin(angle)[:, None, :]
    first = values[..., :half]
    second = values[..., half:]
    return jnp.concatenate(
        [first * cosine - second * sine, second * cosine + first * sine], axis=-1
    )


def sent_to_all(shard, axis):
    size = lax.axis_size(axis)
    return lax.all_to_all(
        jnp.broadcast_to(shard[None], (size, *shard.shape)), axis, 0, 0, tiled=True
    )


def gathered_qkv(place, shard):
    x_hi, x_lo, y, z, core = place
    first = core == 0

    def off_z(k):
        return lambda x, y, z, c: (x, y, z - k, c)

    def z_or_y(k):
        return lambda x, y, z, c: (x, y, z - k, c) if c == 0 else (x, y - k, z, c)

    def y_or_x(k, own):
        def to(x, y, z, c):
            if c == 0:
                return (x, y - k, z, c)
            return (x, y, z, c) if own else (x + 2, y, z, c)

        return to

    slot_a = moved(shard, lambda x, y, z, c: (SWAPPED[x], y, z, c))
    slot_b = moved(slot_a, lambda x, y, z, c: (x + 2, y, z, c) if c == 0 else (x, y, z, c))
    from_z = [slot_a] + [moved(slot_a, off_z(k)) for k in (1, 2, 3)]
    index = [(y - k - z) % 4 for k in range(4)]
    second = [slot_b]
    for k in (1, 2, 3):
        second.append(moved(chosen(jnp.where(first, 4, index[k]), from_z + [slot_b]), z_or_y(k)))
    kept = jnp.stack(
        [chosen(index[0], from_z), chosen(jnp.where(first, index[0], 1), second)]
    )
    sent = [
        jnp.stack(
            [
                chosen(jnp.where(first, index[1], index[0]), from_z),
                chosen(jnp.where(first, index[1], 1), second),
            ]
        ),
        jnp.stack(
            [
                chosen(jnp.where(first, index[2], 4), from_z + [second[2]]),
                chosen(jnp.where(first, index[2], 3), second),
            ]
        ),
        jnp.stack(
            [
                chosen(jnp.where(first, index[3], 4), from_z + [second[2]]),
                chosen(jnp.where(first, index[3], 3), second),
            ]
        ),
    ]
    own = [kept] + [moved(sent[k - 1], y_or_x(k, k == 3)) for k in (1, 2, 3)]
    other = [moved(a, lambda x, y, z, c: (x, y, z, c + 1)) for a in own]
    table_a, table_b = [], []
    for i in range(4):
        for t in range(2):
            table_a.append(4 * (x_hi if t == 0 else 1 - x_hi) + (y + i) % 4)
            low = x_hi if i in (0, 3) else 1 - x_hi
            table_b.append(8 + 4 * low + (y + t + (2 if i > 1 else 0)) % 4)
    table_a, table_b = jnp.stack(table_a), jnp.stack(table_b)
    table = jnp.concatenate(
        [jnp.where(first, table_a, table_b), jnp.where(first, table_b, table_a)]
    )
    return table.astype(jnp.int32), own + other


def gathered_o(place, shard):
    x_hi, _, _, z, core = place
    tp_count = lax.axis_size("tp")
    split = jnp.transpose(shard.reshape(shard.shape[0], tp_count, -1), (1, 0, 2))
    rows = lax.all_to_all(split, "tp", split_axis=0, concat_axis=0, tiled=True)
    rows = rows.reshape(-1, rows.shape[-1])
    across = moved(rows, lambda x, y, z, c: (x + 2, y, z, c))
    pair = jnp.stack([rows, across])
    own = [pair] + [moved(pair, lambda x, y, z, c, k=k: (x, y, z - k, c)) for k in (1, 2, 3)]
    other = [moved(a, lambda x, y, z, c: (x, y, z, c + 1)) for a in own]
    table = []
    for side in range(2):
        at_core = core if side == 0 else 1 - core
        for k in range(4):
            for t in range(2):
                table.append((x_hi if t == 0 else 1 - x_hi) * 8 + ((z + k) % 4) * 2 + at_core)
    return jnp.stack(table).astype(jnp.int32), own + other


def body(
    hidden, positions, key_cache, value_cache, norm_gain, q_proj, k_proj, v_proj, o_proj, post_gain
):
    rep, tp = lax.axis_index("rep"), lax.axis_index("tp")
    place = (rep // 8, tp // 4, tp % 4, (rep // 2) % 4, rep % 2)
    table, pieces = gathered_qkv(place, jnp.concatenate([q_proj, k_proj, v_proj], axis=0))
    joined_block = joined_columns(table, pieces, 512)
    table_o, pieces_o = gathered_o(place, o_proj)
    out_block = wo_rows(table_o, pieces_o, 128)
    batch, kv_local, length, head_dim = key_cache.shape
    group = 2
    q_local = kv_local * group
    q_width, kv_width = q_local * head_dim, kv_local * head_dim
    normed = rms_scale(hidden.astype(jnp.float32), norm_gain).astype(jnp.bfloat16)
    query_key_value_projected = jnp.dot(normed, joined_block, preferred_element_type=jnp.float32)
    query = query_key_value_projected[:, :q_width].reshape(batch, q_local, head_dim)
    keys_new = query_key_value_projected[:, q_width : q_width + kv_width].reshape(
        batch, kv_local, head_dim
    )
    values_new = query_key_value_projected[:, q_width + kv_width :].reshape(
        batch, kv_local, head_dim
    )
    query_rot = rotate(query, positions).astype(jnp.bfloat16)
    rotated_keys = rotate(keys_new, positions).astype(jnp.bfloat16)
    values_rot = values_new.astype(jnp.bfloat16)
    grouped_heads = query_rot.reshape(batch, kv_local, group, head_dim)
    scores = (
        jnp.einsum("bkgd,bkld->bkgl", grouped_heads, key_cache, preferred_element_type=jnp.float32)
        * score_scale
    )
    capped = soft_cap * jnp.tanh(scores / soft_cap)
    valid = jnp.arange(length, dtype=jnp.int32)[None, :] < positions[:, None]
    weight_raw = jnp.where(valid[:, None, None, :], jnp.exp(capped), 0.0)
    self_score = (
        jnp.einsum("juzy,juy->juz", grouped_heads, rotated_keys, preferred_element_type=jnp.float32)
        * score_scale
    )
    self_raw = jnp.exp(soft_cap * jnp.tanh(self_score / soft_cap))
    denom = jnp.sum(weight_raw, axis=-1) + self_raw
    weights = (weight_raw / denom[..., None]).astype(jnp.bfloat16)
    self_weight = (self_raw / denom).astype(jnp.bfloat16)
    attention = jnp.einsum(
        "bkgl,bkld->bkgd", weights, value_cache, preferred_element_type=jnp.float32
    )
    attention = (
        attention
        + self_weight.astype(jnp.float32)[..., None] * values_rot.astype(jnp.float32)[:, :, None, :]
    )
    attention = attention.reshape(batch, q_width).astype(jnp.bfloat16)
    partial_out = jnp.dot(attention, out_block, preferred_element_type=jnp.float32)
    width_local = post_gain.shape[0]
    total = sent_to_all(partial_out, "tp").sum(axis=0)
    multiplier = lax.rsqrt(jnp.mean(total * total, axis=1) + 1e-06)
    share = lax.dynamic_slice_in_dim(total, tp * width_local, width_local, 1)
    result = share * multiplier[:, None] * post_gain
    return (joined_block, out_block, result.astype(jnp.bfloat16))


def solution(mesh):
    in_specs = (
        P("rep", None),
        P("rep"),
        P("rep", "tp", None, None),
        P("rep", "tp", None, None),
        P(),
        P(("rep", "tp"), None),
        P(("rep", "tp"), None),
        P(("rep", "tp"), None),
        P(("rep", "tp"), None),
        P("tp"),
    )
    out_specs = (P(None, "tp"), P("tp", None), P("rep", "tp"))
    return jax.shard_map(body, mesh=mesh, in_specs=in_specs, out_specs=out_specs, check_vma=False)
```

```python
import functools

import jax
import jax.numpy as jnp
from jax import lax
from jax.experimental import pallas as pl
from jax.experimental.pallas import tpu as pltpu
from jax.sharding import PartitionSpec as P

score_scale = 144.0 ** (-0.5)
soft_cap = 50.0
AXES = ("xh", "z", "c", "xl", "y")
REP = ("xh", "z", "c")
TP = ("xl", "y")


def flat_index(x, y, z, c):
    x, y, z, c = x % 4, y % 4, z % 4, c % 2
    return ((x // 2) * 8 + z * 2 + c) * 8 + (x % 2) * 4 + y


def moved(value, to):
    pairs = []
    for x in range(4):
        for y in range(4):
            for z in range(4):
                for c in range(2):
                    pairs.append((flat_index(x, y, z, c), flat_index(*to(x, y, z, c))))
    return lax.ppermute(value, AXES, pairs)


SWAPPED = (0, 2, 1, 3)


def picked_kernel(counts, index, *refs):
    sources, out, held, arrived, left = refs[: sum(counts)], *refs[sum(counts) :]
    start = 0
    for part, count in enumerate(counts):
        for k in range(count):

            @pl.when(index[part] == k)
            def _():
                pltpu.make_async_copy(
                    sources[start + k], held.at[part], arrived.at[part]
                ).start()

        start += count
    for part in range(len(counts)):
        pltpu.make_async_copy(sources[0], held.at[part], arrived.at[part]).wait()
        pltpu.make_async_copy(held.at[part], out.at[part], left.at[part]).start()
    for part in range(len(counts)):
        pltpu.make_async_copy(held.at[part], out.at[part], left.at[part]).wait()


def picked(index, options):
    counts = tuple(len(o) for o in options)
    flat = [a for o in options for a in o]
    parts = len(options)
    shape = (parts, *flat[0].shape)
    hbm = pl.BlockSpec(memory_space=pltpu.HBM)
    return pl.pallas_call(
        functools.partial(picked_kernel, counts),
        out_shape=jax.ShapeDtypeStruct(shape, flat[0].dtype),
        grid_spec=pltpu.PrefetchScalarGridSpec(
            num_scalar_prefetch=1,
            grid=(1,),
            in_specs=[hbm] * len(flat),
            out_specs=hbm,
            scratch_shapes=[
                pltpu.VMEM(shape, flat[0].dtype),
                pltpu.SemaphoreType.DMA((parts,)),
                pltpu.SemaphoreType.DMA((parts,)),
            ],
        ),
        cost_estimate=pl.CostEstimate(
            flops=4000000, bytes_accessed=4 * flat[0].size * parts, transcendentals=0
        ),
        name="picked",
    )(jnp.stack(index).astype(jnp.int32), *flat)


def unit(size):
    row = lax.broadcasted_iota(jnp.int32, (size, size), 0)
    column = lax.broadcasted_iota(jnp.int32, (size, size), 1)
    return (row == column).astype(jnp.bfloat16)


def turned(rows, out, step):
    eye = unit(step)
    for d in range(0, rows.shape[1], step):
        turned_step = lax.dot_general(
            eye, rows[:, d : d + step], (((1,), (1,)), ((), ())), preferred_element_type=jnp.float32
        )
        out[d : d + step, :] = turned_step.astype(jnp.bfloat16)


def joined_kernel(table, *refs):
    pieces, out, rows = refs[:8], refs[8], refs[9]
    for i in range(8):
        for t in range(2):
            place = table[2 * i + t]
            q_at = pl.multiple_of(place * 32, 32)
            kv_at = pl.multiple_of(place * 16, 16)
            rows[pl.ds(q_at, 32), :] = pieces[i][t, 0:32, :]
            rows[pl.ds(512 + kv_at, 16), :] = pieces[i][t, 32:48, :]
            rows[pl.ds(768 + kv_at, 16), :] = pieces[i][t, 48:64, :]
    turned(rows, out, 256)


def wo_kernel(table, *refs):
    count = len(refs) - 2
    pieces, out, rows = refs[:count], refs[count], refs[count + 1]
    parts, height, _ = pieces[0].shape
    for i in range(count):
        for t in range(parts):
            at = pl.multiple_of(table[parts * i + t] * height, 16)
            rows[pl.ds(at, height), :] = pieces[i][t]
    turned(rows, out, 256)


def assembled(kernel, table, pieces, chunk, name):
    parts, height, width = pieces[0].shape
    block = pl.BlockSpec((parts, height, chunk), lambda d, *_: (0, 0, d))
    total = height * parts * len(pieces)
    return pl.pallas_call(
        kernel,
        out_shape=jax.ShapeDtypeStruct((width, total), jnp.bfloat16),
        grid_spec=pltpu.PrefetchScalarGridSpec(
            num_scalar_prefetch=1,
            grid=(width // chunk,),
            in_specs=[block] * len(pieces),
            out_specs=pl.BlockSpec((chunk, total), lambda d, *_: (d, 0)),
            scratch_shapes=[pltpu.VMEM((total, chunk), jnp.bfloat16)],
        ),
        cost_estimate=pl.CostEstimate(
            flops=512 * width * total, bytes_accessed=4 * width * total, transcendentals=0
        ),
        name=name,
    )(table, *pieces)


def rms_scale(values, gain):
    mean_square = jnp.mean(values * values, axis=-1, keepdims=True)
    return values * lax.rsqrt(mean_square + 1e-06) * gain


def rotate(values, positions):
    half = values.shape[-1] // 2
    freq = 10000.0 ** (-2.0 * jnp.arange(half, dtype=jnp.float32) / values.shape[-1])
    angle = positions.astype(jnp.float32)[:, None] * freq[None, :]
    cosine = jnp.cos(angle)[:, None, :]
    sine = jnp.sin(angle)[:, None, :]
    first = values[..., :half]
    second = values[..., half:]
    return jnp.concatenate(
        [first * cosine - second * sine, second * cosine + first * sine], axis=-1
    )


def sent_to_all(shard, axis):
    size = lax.axis_size(axis)
    return lax.all_to_all(
        jnp.broadcast_to(shard[None], (size, *shard.shape)), axis, 0, 0, tiled=True
    )


def z_copies(value):
    return [value] + [moved(value, lambda x, y, z, c, k=k: (x, y, z - k, c)) for k in (1, 2, 3)]


def to_partner(value):
    return moved(value, lambda x, y, z, c: (x, y, z, c + 1))


def across(value):
    return moved(value, lambda x, y, z, c: (x + 2, y, z, c))


def gathered_qkv(place, slot_a, slot_b, from_z):
    x_hi, x_lo, y, z, core = place
    first = core == 0

    def z_or_y(k):
        return lambda x, y, z, c: (x, y, z - k, c) if c == 0 else (x, y - k, z, c)

    def y_or_x(k, own):
        def to(x, y, z, c):
            if c == 0:
                return (x, y - k, z, c)
            return (x, y, z, c) if own else (x + 2, y, z, c)

        return to

    index = [(y - k - z) & 3 for k in range(4)]
    second = [slot_b]
    for k in (1, 2, 3):
        operand = picked([jnp.where(first, 4, index[k])], [from_z + [slot_b]])[0]
        second.append(moved(operand, z_or_y(k)))
    wide = from_z + [second[2]]
    sent = [
        picked([index[0], jnp.where(first, index[0], 1)], [from_z, second]),
        picked(
            [jnp.where(first, index[1], index[0]), jnp.where(first, index[1], 1)],
            [from_z, second],
        ),
        picked([jnp.where(first, index[2], 4), jnp.where(first, index[2], 3)], [wide, second]),
        picked([jnp.where(first, index[3], 4), jnp.where(first, index[3], 3)], [wide, second]),
    ]
    own = [sent[0]] + [moved(sent[k], y_or_x(k, k == 3)) for k in (1, 2, 3)]
    other = [to_partner(a) for a in own]
    table_a, table_b = [], []
    for i in range(4):
        for t in range(2):
            table_a.append(4 * (x_hi if t == 0 else 1 - x_hi) + ((y + i) & 3))
            low = x_hi if i in (0, 3) else 1 - x_hi
            table_b.append(8 + 4 * low + ((y + t + (2 if i > 1 else 0)) & 3))
    table_a, table_b = jnp.stack(table_a), jnp.stack(table_b)
    table = jnp.concatenate(
        [jnp.where(first, table_a, table_b), jnp.where(first, table_b, table_a)]
    )
    return table.astype(jnp.int32), own + other


def gathered_o(place, shard):
    x_hi, _, _, z, core = place
    tp_count = lax.axis_size(TP)
    stacked = jnp.stack(z_copies(shard))
    copies, height, width = stacked.shape
    split = jnp.transpose(stacked.reshape(copies, height, tp_count, -1), (2, 0, 1, 3))
    rows = lax.all_to_all(split, TP, split_axis=0, concat_axis=0, tiled=True)
    rows = jnp.transpose(rows, (1, 0, 2, 3)).reshape(copies, tp_count * height, -1)
    own = [rows, across(rows)]
    other = [to_partner(a) for a in own]
    table = []
    for side in range(2):
        at_core = core if side == 0 else 1 - core
        for t in range(2):
            for k in range(4):
                table.append((x_hi if t == 0 else 1 - x_hi) * 8 + ((z + k) & 3) * 2 + at_core)
    return jnp.stack(table).astype(jnp.int32), own + other


def new_token(place, every, from_z, width_q, width_kv):
    z = place[3]
    products = [
        lax.dot_general(
            every, piece, (((1,), (1,)), ((), ())), preferred_element_type=jnp.float32
        )
        for piece in from_z
    ]
    both = jnp.stack(products + products)
    by_y = lax.dynamic_slice_in_dim(both, (4 - z) & 3, 4, 0)
    columns = by_y.shape[-1]
    sent = jnp.transpose(by_y.reshape(4, 4, -1, columns), (1, 0, 2, 3)).reshape(16, -1, columns)
    came = lax.all_to_all(sent, ("xh", "c", "y"), split_axis=0, concat_axis=0, tiled=True)
    came = jnp.transpose(came.reshape(2, 2, 4, -1, columns), (3, 1, 0, 2, 4))
    batch = came.shape[0]
    a, b = columns // 2, columns * 3 // 4
    return tuple(
        part.reshape(batch, -1) for part in (came[..., :a], came[..., a:b], came[..., b:])
    )


def body(
    hidden, positions, key_cache, value_cache, norm_gain, q_proj, k_proj, v_proj, o_proj, post_gain
):
    x_hi, z, core, x_lo, y = (lax.axis_index(name) for name in AXES)
    place = (x_hi, x_lo, y, z, core)
    tp = x_lo * 4 + y
    batch, kv_local, length, head_dim = key_cache.shape
    group = 2
    q_local = kv_local * group
    q_width, kv_width = q_local * head_dim, kv_local * head_dim

    shard = jnp.concatenate([q_proj, k_proj, v_proj], axis=0)
    slot_a = moved(shard, lambda x, y, z, c: (SWAPPED[x], y, z, c))
    normed = rms_scale(hidden.astype(jnp.float32), norm_gain).astype(jnp.bfloat16)
    every = sent_to_all(normed, ("xh", "c")).reshape(-1, normed.shape[-1])
    from_z = z_copies(slot_a)
    slot_b = moved(slot_a, lambda x, y, z, c: (x + 2, y, z, c) if c == 0 else (x, y, z, c))
    table_o, pieces_o = gathered_o(place, o_proj)
    out_block = assembled(wo_kernel, table_o, pieces_o, 256, "wo")
    table, pieces = gathered_qkv(place, slot_a, slot_b, from_z)
    joined_block = assembled(joined_kernel, table, pieces, 2304, "joined")

    query, keys_new, values_new = new_token(place, every, from_z, q_width, kv_width)
    query = query.reshape(batch, q_local, head_dim)
    keys_new = keys_new.reshape(batch, kv_local, head_dim)
    values_new = values_new.reshape(batch, kv_local, head_dim)
    query_rot = rotate(query, positions).astype(jnp.bfloat16)
    rotated_keys = rotate(keys_new, positions).astype(jnp.bfloat16)
    values_rot = values_new.astype(jnp.bfloat16)
    grouped_heads = query_rot.reshape(batch, kv_local, group, head_dim)
    scores = (
        jnp.einsum("bkgd,bkld->bkgl", grouped_heads, key_cache, preferred_element_type=jnp.float32)
        * score_scale
    )
    capped = soft_cap * jnp.tanh(scores / soft_cap)
    valid = jnp.arange(length, dtype=jnp.int32)[None, :] < positions[:, None]
    weight_raw = jnp.where(valid[:, None, None, :], jnp.exp(capped), 0.0)
    self_score = (
        jnp.einsum("juzy,juy->juz", grouped_heads, rotated_keys, preferred_element_type=jnp.float32)
        * score_scale
    )
    self_raw = jnp.exp(soft_cap * jnp.tanh(self_score / soft_cap))
    denom = jnp.sum(weight_raw, axis=-1) + self_raw
    weights = (weight_raw / denom[..., None]).astype(jnp.bfloat16)
    self_weight = (self_raw / denom).astype(jnp.bfloat16)
    attention = jnp.einsum(
        "bkgl,bkld->bkgd", weights, value_cache, preferred_element_type=jnp.float32
    )
    attention = (
        attention
        + self_weight.astype(jnp.float32)[..., None] * values_rot.astype(jnp.float32)[:, :, None, :]
    )
    attention = attention.reshape(batch, q_width).astype(jnp.bfloat16)
    partial_out = jnp.dot(attention, out_block, preferred_element_type=jnp.float32)
    width_local = post_gain.shape[0]
    total = sent_to_all(partial_out, TP).sum(axis=0)
    multiplier = lax.rsqrt(jnp.mean(total * total, axis=1) + 1e-06)
    share = lax.dynamic_slice_in_dim(total, tp * width_local, width_local, 1)
    result = share * multiplier[:, None] * post_gain
    return (joined_block, out_block, result.astype(jnp.bfloat16))


def solution(mesh):
    split = jax.sharding.Mesh(mesh.devices.reshape(2, 4, 2, 2, 4), AXES)
    in_specs = (
        P(REP, None),
        P(REP),
        P(REP, TP, None, None),
        P(REP, TP, None, None),
        P(),
        P(AXES, None),
        P(AXES, None),
        P(AXES, None),
        P(AXES, None),
        P(TP),
    )
    out_specs = (P(None, TP), P(TP, None), P(REP, TP))
    return jax.shard_map(body, mesh=split, in_specs=in_specs, out_specs=out_specs, check_vma=False)
```
